32 devices in a mesh: seg: 4 (over z), cp: 8 (over y, x, core).
Axes of the slice: x: 2, y: 2, z: 4, core: 2. Of those that a mesh axis runs over, the one named last changes fastest.
Arguments:
- mixed_qkv: bfloat16 [4096, 8192], P(('seg', 'cp')), may hold values from -6 to 6
- gate_z: bfloat16 [4096, 4096], P(('seg', 'cp')), may hold values from -6 to 6
- gate_logits: bfloat16 [4096, 64], P(('seg', 'cp')), may hold values from -16 to 4
- block_table: int32 [4, 16], P('seg'), may hold values from 0 to 15, as said below
- conv_weight: float32 [4, 8192], replicated, may hold values from -3 to 3
- a_log: float32 [32], replicated, may hold values from -0.7 to 0.7
- dt_bias: float32 [32], replicated, may hold values from -0.5 to 0.5
- norm_gain: float32 [128], replicated, may hold values from 0.25 to 1.75
Outputs:
- mixed_out: bfloat16 [4096, 4096], P(('seg', 'cp'))
The draws below stay inside these ranges and needn't reach their ends.
Inputs may be any that keep to these rules, and one draw needn't show every extreme that they name: Each row of block_table is a permutation of the numbers 0 to 15; its entries at even positions are below 8, those at odd positions are 8 or more.
All inputs are finite; a program needn't handle non-finite values.
Results may differ from the reference program's by a relative error of at most 0.001.
Values may be sent and summed in bfloat16 or wider, within the bound.
A program may use at most 128 MiB of HBM per device.

```python
import jax
import jax.numpy as jnp
from jax import lax

VALUE_HEADS = 32
KEY_HEADS = 16
HEAD_DIM = 128
CONV = 4
BLOCK = 128
TOK_DEV = 128
SEQUENCE_TOKENS = 4096
N_SEG = 4
N_CP = 8


def draw_gate_logits(key, part):
    random_subkeys = jax.random.split(key, 9)
    slow_share = 0.5
    beta_noise = 0.5 * jax.random.normal(random_subkeys[4], (SEQUENCE_TOKENS, VALUE_HEADS), jnp.float32)
    slow_heads = jax.random.uniform(random_subkeys[0], (VALUE_HEADS,), jnp.float32) < slow_share
    beta_base = jnp.where(slow_heads, jax.random.uniform(random_subkeys[1], (VALUE_HEADS,), jnp.float32, -7.0, -5.0), jax.random.uniform(random_subkeys[2], (VALUE_HEADS,), jnp.float32, -1.0, 2.0))
    decay_base = jnp.where(slow_heads, jax.random.uniform(random_subkeys[3], (VALUE_HEADS,), jnp.float32, -13.0, -11.0), jax.random.uniform(random_subkeys[5], (VALUE_HEADS,), jnp.float32, -4.0, -3.0))
    rows_per_half = TOK_DEV // 2
    group_count = SEQUENCE_TOKENS // rows_per_half
    offsets = jax.random.uniform(random_subkeys[6], (group_count, 1, VALUE_HEADS), jnp.float32, -0.7, 0.7)
    offsets = jnp.broadcast_to(offsets, (group_count, rows_per_half, VALUE_HEADS)).reshape(SEQUENCE_TOKENS, VALUE_HEADS)
    beta_logit = beta_base + beta_noise
    decay_logit_raw = decay_base + offsets + 0.3 * jax.random.normal(random_subkeys[7], (SEQUENCE_TOKENS, VALUE_HEADS), jnp.float32)
    doubling_rows = jax.random.uniform(random_subkeys[8], (SEQUENCE_TOKENS, 1), jnp.float32) < 6.0 / SEQUENCE_TOKENS
    doubling_level = jax.random.uniform(jax.random.fold_in(random_subkeys[8], 7), (SEQUENCE_TOKENS, VALUE_HEADS), jnp.float32, -1.0, 0.0)
    decay_logit_raw = jnp.where(doubling_rows, jnp.maximum(decay_logit_raw, doubling_level), decay_logit_raw)
    joined = jnp.concatenate([beta_logit, decay_logit_raw], axis=1)
    return jnp.clip(joined, -16.0, 4.0).astype(jnp.bfloat16)


def draw_block_table(key, part):
    base = jax.random.fold_in(key, 41)
    first_keys = jax.random.split(jax.random.fold_in(base, 1), N_SEG)
    second_keys = jax.random.split(jax.random.fold_in(base, 2), N_SEG)
    first = jax.vmap(lambda one: jax.random.permutation(one, N_CP))(first_keys).astype(jnp.int32)
    second = jax.vmap(lambda one: jax.random.permutation(one, N_CP))(second_keys).astype(jnp.int32) + N_CP
    return jnp.stack([first, second], axis=-1).reshape(N_SEG, 2 * N_CP).astype(jnp.int32)


def levels(own_key, shape, cuts, least, largest):
    factor_of = 1.0
    for position, blocks in cuts:
        draws = jax.random.uniform(jax.random.fold_in(jax.random.fold_in(own_key, 6), position), (blocks,), jnp.float32, least / len(cuts), largest / len(cuts))
        factor_of = factor_of * jnp.repeat(jnp.exp(draws), shape[position] // blocks).reshape((-1,) + (1,) * (len(shape) - 1 - position))
    return factor_of


def normal_values(own_key, shape, deviation, most, cuts=(), kind=jnp.bfloat16):
    factor_of = levels(own_key, shape, cuts, -0.22, 0.18) if cuts else 1.0
    values = jax.random.normal(own_key, shape, jnp.float32) * deviation * factor_of
    return jnp.minimum(jnp.maximum(values, -most), most).astype(kind)


def setup_inputs(seed: int = 0) -> dict:
    seeds = jax.random.split(jax.random.key(seed), 9)
    return {
        "mixed_qkv": normal_values(seeds[0], (SEQUENCE_TOKENS, 2 * KEY_HEADS * HEAD_DIM + VALUE_HEADS * HEAD_DIM), 1.0, 6.0, ((0, 32),)),
        "gate_z": normal_values(seeds[1], (SEQUENCE_TOKENS, VALUE_HEADS * HEAD_DIM), 1.0, 6.0, ((0, 32),)),
        "gate_logits": draw_gate_logits(jax.random.fold_in(seeds[8], 71), 0),
        "block_table": draw_block_table(jax.random.fold_in(seeds[8], 71), 0),
        "conv_weight": normal_values(seeds[4], (CONV, 2 * KEY_HEADS * HEAD_DIM + VALUE_HEADS * HEAD_DIM), CONV ** -0.5, 3.0, (), jnp.float32),
        "a_log": jnp.clip(jax.random.uniform(seeds[5], (VALUE_HEADS,), jnp.float32, -0.7, 0.7), -0.7, 0.7),
        "dt_bias": jnp.clip(jax.random.uniform(seeds[6], (VALUE_HEADS,), jnp.float32, -0.5, 0.5), -0.5, 0.5),
        "norm_gain": jnp.clip(1.0 + 0.15 * jax.random.normal(seeds[7], (HEAD_DIM,), jnp.float32), 0.25, 1.75),
    }


highest = lax.Precision.HIGHEST

def to_sequence(stored, table):
    columns = stored.shape[1]
    pieces = stored.reshape(N_SEG, 2 * N_CP, TOK_DEV // 2, columns)
    order = jnp.argsort(table, axis=1).astype(jnp.int32)
    picked = jnp.take_along_axis(pieces, order[:, :, None, None], axis=1)
    return picked.reshape(stored.shape[0], columns)

def causal_conv(rows, weights):
    padded = jnp.pad(rows, ((CONV - 1, 0), (0, 0)))
    length = rows.shape[0]
    summed = jnp.zeros(rows.shape, jnp.float32)
    for offset in range(CONV):
        summed = summed + weights[offset] * padded[offset:offset + length].astype(jnp.float32)
    return jax.nn.silu(summed)

def unit_rows(matrix):
    return matrix * lax.rsqrt(lax.optimization_barrier(jnp.sum(matrix * matrix, axis=-1, keepdims=True)) + 1e-06)

def block_terms(queries, key_rows, values, beta_rate, decays):
    cumulative = jnp.cumsum(decays, axis=-1)
    final_sum = cumulative[..., -1:]
    spread = cumulative[..., :, None] - cumulative[..., None, :]
    row_index = lax.broadcasted_iota(jnp.int32, (BLOCK, BLOCK), 0)
    col_index = lax.broadcasted_iota(jnp.int32, (BLOCK, BLOCK), 1)
    strict = row_index > col_index
    inclusive = row_index >= col_index
    strict_decay = jnp.where(strict, jnp.exp(jnp.where(strict, spread, 0.0)), 0.0)
    incl_decay = jnp.where(inclusive, jnp.exp(jnp.where(inclusive, spread, 0.0)), 0.0)
    weighted = key_rows * beta_rate[..., None]
    lower = jnp.einsum('...cd,...ed->...ce', weighted, key_rows, precision=highest) * strict_decay
    system = lower + jnp.eye(BLOCK, dtype=jnp.float32)
    right_side = jnp.concatenate([values * beta_rate[..., None], weighted * jnp.exp(cumulative)[..., None]], axis=-1)
    solved = jax.scipy.linalg.solve_triangular(system, right_side, lower=True, unit_diagonal=True)
    corrected = solved[..., :HEAD_DIM]
    projector = solved[..., HEAD_DIM:]
    key_decay = key_rows * jnp.exp(final_sum - cumulative)[..., None]
    query_decay = queries * jnp.exp(cumulative)[..., None]
    scores = jnp.einsum('...cd,...ed->...ce', queries, key_rows, precision=highest) * incl_decay
    return (corrected, projector, key_decay, query_decay, scores, jnp.exp(final_sum[..., 0]))

def reference(mixed_qkv, gate_z, gate_logits, block_table, conv_weight, a_log, dt_bias, norm_gain):
    seq_qkv = to_sequence(mixed_qkv, block_table)
    seq_z = to_sequence(gate_z, block_table)
    seq_gates = to_sequence(gate_logits, block_table)
    conv_out = causal_conv(seq_qkv, conv_weight)
    length = conv_out.shape[0]
    key_width = KEY_HEADS * HEAD_DIM
    group_size = VALUE_HEADS // KEY_HEADS
    queries = unit_rows(conv_out[:, :key_width].reshape(length, KEY_HEADS, HEAD_DIM)) * HEAD_DIM ** (-0.5)
    key_rows = unit_rows(conv_out[:, key_width:2 * key_width].reshape(length, KEY_HEADS, HEAD_DIM))
    queries = jnp.repeat(queries, group_size, axis=1)
    key_rows = jnp.repeat(key_rows, group_size, axis=1)
    values = conv_out[:, 2 * key_width:].reshape(length, VALUE_HEADS, HEAD_DIM)
    gate_float = seq_gates.astype(jnp.float32)
    beta_rate = jax.nn.sigmoid(gate_float[:, :VALUE_HEADS])
    decays = -jnp.exp(a_log) * jax.nn.softplus(gate_float[:, VALUE_HEADS:] + dt_bias)
    count = length // BLOCK

    def to_blocks(array):
        return array.reshape(count, BLOCK, VALUE_HEADS, HEAD_DIM).transpose(0, 2, 1, 3)

    def to_block_rates(array):
        return array.reshape(count, BLOCK, VALUE_HEADS).transpose(0, 2, 1)

    def block_step(state, pieces):
        query_block, key_block, value_block, beta_block, decay_block = pieces
        corrected, projector, key_decay, query_decay, scores, last_decay = block_terms(query_block, key_block, value_block, beta_block, decay_block)
        new_values = corrected - jnp.einsum('hcd,hde->hce', projector, state, precision=highest)
        outputs = jnp.einsum('hcd,hde->hce', query_decay, state, precision=highest)
        outputs = outputs + jnp.einsum('hce,hev->hcv', scores, new_values, precision=highest)
        state = last_decay[:, None, None] * state + jnp.einsum('hcd,hce->hde', key_decay, new_values, precision=highest)
        return (state, outputs)
    initial = jnp.zeros((VALUE_HEADS, HEAD_DIM, HEAD_DIM), jnp.float32)
    _, blocked = lax.scan(block_step, initial, (to_blocks(queries), to_blocks(key_rows), to_blocks(values), to_block_rates(beta_rate), to_block_rates(decays)))
    core = blocked.transpose(0, 2, 1, 3).reshape(length, VALUE_HEADS, HEAD_DIM)
    gate_values = seq_z.astype(jnp.float32).reshape(length, VALUE_HEADS, HEAD_DIM)
    scale = lax.rsqrt(lax.optimization_barrier(jnp.mean(core * core, axis=-1, keepdims=True)) + 1e-06)
    normed = core * scale * norm_gain * jax.nn.silu(gate_values)
    return normed.reshape(length, VALUE_HEADS * HEAD_DIM).astype(jnp.bfloat16)
```

```python
import functools

import jax
import jax.numpy as jnp
from jax import lax
from jax.experimental import pallas as pl
from jax.experimental.pallas import tpu as pltpu
from jax.sharding import PartitionSpec as P

VALUE_HEADS = 32
KEY_HEADS = 16
HEAD_DIM = 128
CONV = 4
BLOCK = 128
TAIL = 16
GROUP = VALUE_HEADS // KEY_HEADS

f32 = jnp.float32
bf16 = jnp.bfloat16
MESH = pl.DeviceIdType.MESH
highest = lax.Precision.HIGHEST


def split(x):
    hi = x.astype(bf16)
    return hi, (x - hi.astype(f32)).astype(bf16)


NN = (((1,), (0,)), ((), ()))
NT = (((1,), (1,)), ((), ()))


def mm(a, b, dims=NN):
    def dot(x, y):
        return lax.dot_general(x, y, dims, preferred_element_type=f32)

    return dot(a[0], b[0]) + (dot(a[0], b[1]) + dot(a[1], b[0]))


def scatter_kernel(n, segs, heads, qkv, z, gates, oq, ok, ov, oz, og, otail, send, recv, local):
    me = lax.axis_index("cp")
    seg = lax.axis_index("seg")
    after = lax.rem(seg + 1, segs)
    before = lax.rem(seg + segs - 1, segs)
    keys = max(1, heads // GROUP)
    wk, wv = keys * HEAD_DIM, heads * HEAD_DIM
    key_width = KEY_HEADS * HEAD_DIM
    rows = qkv.shape[0]

    barrier = pltpu.get_barrier_semaphore()
    for d in range(n):
        peer = lax.rem(me + d, n)
        if d:
            pl.semaphore_signal(barrier, inc=1, device_id=(seg, peer), device_id_type=MESH)
        pl.semaphore_signal(barrier, inc=1, device_id=(before, peer), device_id_type=MESH)
    pl.semaphore_wait(barrier, 2 * n - 1)

    def columns(start, width):
        return pl.ds(pl.multiple_of(start, HEAD_DIM), width)

    def pieces(p, slot):
        kcol = lax.div(p * heads, GROUP) * HEAD_DIM
        vcol = p * wv
        return [
            (qkv.at[:, columns(kcol, wk)], oq.at[slot]),
            (qkv.at[:, columns(key_width + kcol, wk)], ok.at[slot]),
            (qkv.at[:, columns(2 * key_width + vcol, wv)], ov.at[slot]),
            (gates, og.at[slot]),
            (z.at[:, columns(vcol, wv)], oz.at[slot]),
        ]

    def tails(p, slot):
        kcol = lax.div(p * heads, GROUP) * HEAD_DIM
        vcol = p * wv
        last = pl.ds(rows - TAIL, TAIL)
        return [
            (qkv.at[last, columns(kcol, wk)], otail.at[slot, :, pl.ds(0, wk)]),
            (qkv.at[last, columns(key_width + kcol, wk)], otail.at[slot, :, pl.ds(wk, wk)]),
            (qkv.at[last, columns(2 * key_width + vcol, wv)], otail.at[slot, :, pl.ds(2 * wk, wv)]),
        ]

    started = []

    def post(kind, src, dst, peer, target):
        copy = pltpu.make_async_remote_copy(
            src_ref=src,
            dst_ref=dst,
            send_sem=send.at[kind, peer],
            recv_sem=recv.at[kind, me],
            device_id=target,
            device_id_type=MESH,
        )
        copy.start()
        started.append(copy)

    order = sorted(range(1, n), key=lambda d: -min(d, n - d))
    for kinds in ((0, 1, 2, 3), (4,)):
        for d in order:
            peer = lax.rem(me + d, n)
            for kind in kinds:
                src, dst = pieces(peer, me)[kind]
                post(kind, src, dst, peer, (seg, peer))
        if kinds[0] == 0:
            for d in range(n):
                peer = lax.rem(me + d, n)
                for i, (src, dst) in enumerate(tails(peer, me)):
                    post(5 + i, src, dst, peer, (after, peer))
    own = []
    for kind, (src, dst) in enumerate(pieces(me, me)):
        copy = pltpu.make_async_copy(src, dst, local.at[kind])
        copy.start()
        own.append(copy)
    for copy in own:
        copy.wait()
    for d in range(n):
        source = lax.rem(me + n - d, n)
        found = list(enumerate(pieces(me, source))) if d else []
        found += [(5 + i, pair) for i, pair in enumerate(tails(me, source))]
        for kind, (src, dst) in found:
            pltpu.make_async_remote_copy(
                src_ref=src,
                dst_ref=dst,
                send_sem=send.at[kind, source],
                recv_sem=recv.at[kind, source],
                device_id=(seg, source),
                device_id_type=MESH,
            ).wait_recv()
    for copy in started:
        copy.wait_send()


def scatter(n, segs, heads, qkv, z, gates):
    keys = max(1, heads // GROUP)
    wk, wv = keys * HEAD_DIM, heads * HEAD_DIM
    rows = qkv.shape[0]

    def shape(*dims):
        return jax.ShapeDtypeStruct(dims, bf16)

    return pl.pallas_call(
        functools.partial(scatter_kernel, n, segs, heads),
        out_shape=(
            shape(n, rows, wk),
            shape(n, rows, wk),
            shape(n, rows, wv),
            shape(n, rows, wv),
            shape(n, rows, gates.shape[1]),
            shape(n, TAIL, 2 * wk + wv),
        ),
        in_specs=[pl.BlockSpec(memory_space=pl.ANY)] * 3,
        out_specs=[pl.BlockSpec(memory_space=pltpu.VMEM)] * 6,
        scratch_shapes=[
            pltpu.SemaphoreType.DMA((8, n)),
            pltpu.SemaphoreType.DMA((8, n)),
            pltpu.SemaphoreType.DMA((5,)),
        ],
        compiler_params=pltpu.CompilerParams(collective_id=0, has_side_effects=True),
        name="scatter",
    )(qkv, z, gates)


def log1p_exact(y):
    u = 1.0 + y
    return jnp.where(u == 1.0, y, jnp.log(u) * (y / jnp.where(u == 1.0, 1.0, u - 1.0)))


def local_kernel(
    heads, meta, q_ref, k_ref, v_ref, g_ref, tail_ref, w_ref, rate_ref, o_ref, m_ref, end_ref, x_ref, st_ref
):
    keys = max(1, heads // GROUP)
    wk, wv = keys * HEAD_DIM, heads * HEAD_DIM
    total = 2 * pl.num_programs(0)
    b = pl.program_id(0)
    i0 = meta[2 * b]
    i1 = meta[2 * b + 1]
    ip = meta[jnp.maximum(2 * b - 1, 0)]
    tail_from = meta[total]
    no_tail = meta[total + 1]
    head_start = meta[total + 2]
    half = q_ref.shape[1]

    row = lax.broadcasted_iota(jnp.int32, (BLOCK, BLOCK), 0)
    col = lax.broadcasted_iota(jnp.int32, (BLOCK, BLOCK), 1)
    strict = row > col
    inclusive = row >= col
    eye = jnp.where(row == col, 1.0, 0.0).astype(f32)

    @pl.when(b == 0)
    def _():
        for h in range(heads):
            st_ref[h, :, :HEAD_DIM] = jnp.zeros((HEAD_DIM, HEAD_DIM), f32)
            st_ref[h, :, HEAD_DIM:] = eye

    tail_rows = jnp.where(no_tail > 0, 0.0, tail_ref[tail_from].astype(f32))[TAIL - 8 :]
    at = 0
    for ref, width in ((q_ref, wk), (k_ref, wk), (v_ref, wv)):
        cols = slice(at, at + width)
        prior = ref[ip, half - 16 :, :].astype(f32)[8:]
        x_ref[0:8, cols] = jnp.where(b == 0, tail_rows[:, cols], prior)
        x_ref[8 : 8 + half, cols] = ref[i0].astype(f32)
        x_ref[8 + half : 8 + 2 * half, cols] = ref[i1].astype(f32)
        at += width

    def conv(start):
        cols = slice(start, start + HEAD_DIM)
        total_rows = w_ref[0:1, cols] * x_ref[5 : 5 + BLOCK, cols]
        for j in range(1, CONV):
            total_rows = total_rows + w_ref[j : j + 1, cols] * x_ref[5 + j : 5 + j + BLOCK, cols]
        return total_rows / (1.0 + jnp.exp(-total_rows))

    def unit(x):
        return x * lax.rsqrt(jnp.sum(x * x, axis=-1, keepdims=True) + 1e-06)

    gates = jnp.concatenate([g_ref[i0], g_ref[i1]], axis=0).astype(f32)
    gates = jnp.concatenate([gates, jnp.zeros((BLOCK, BLOCK - gates.shape[1]), f32)], axis=1)
    beta_all = 1.0 / (1.0 + jnp.exp(-gates))
    shifted = gates + rate_ref[1:2, :]
    soft = jnp.maximum(shifted, 0.0) + log1p_exact(jnp.exp(-jnp.abs(shifted)))
    decays = rate_ref[0:1, :] * soft
    turn = lax.rem(BLOCK - head_start, BLOCK)
    beta_all = pltpu.roll(beta_all, turn, 1)
    decays = pltpu.roll(decays, turn, 1)
    tril = jnp.where(inclusive, 1.0, 0.0).astype(bf16)
    d0 = decays.astype(bf16)
    rest = decays - d0.astype(f32)
    d1 = rest.astype(bf16)
    d2 = (rest - d1.astype(f32)).astype(bf16)
    cum = jnp.dot(tril, d2, preferred_element_type=f32)
    cum = cum + jnp.dot(tril, d1, preferred_element_type=f32)
    cum = cum + jnp.dot(tril, d0, preferred_element_type=f32)
    cum_t = jnp.transpose(cum)

    queries, key_rows, kk, qk = [], [], [], []
    for g in range(keys):
        queries.append(unit(conv(g * HEAD_DIM)) * HEAD_DIM ** (-0.5))
        key_rows.append(unit(conv(wk + g * HEAD_DIM)))
        ks = split(key_rows[g])
        qs = split(queries[g])
        kk.append(mm(ks, ks, NT))
        qk.append(mm(qs, ks, NT))

    hs = range(heads)
    lower, scores, rhs, kdt, qd, last = [], [], [], [], [], []
    for h in hs:
        g = h * keys // heads
        beta = beta_all[:, h : h + 1]
        c = cum[:, VALUE_HEADS + h : VALUE_HEADS + h + 1]
        ct = cum_t[VALUE_HEADS + h : VALUE_HEADS + h + 1, :]
        final = ct[:, BLOCK - 1 :]
        spread = c - ct
        incl = jnp.where(inclusive, jnp.exp(jnp.where(inclusive, spread, 0.0)), 0.0)
        lower.append(jnp.where(strict, beta * kk[g] * incl, 0.0))
        scores.append(split(qk[g] * incl))
        grow = jnp.exp(c)
        values = conv(2 * wk + h * HEAD_DIM)
        rhs.append(split(jnp.concatenate([values * beta, key_rows[g] * (beta * grow)], axis=1)))
        kdt.append(split(jnp.transpose(key_rows[g] * jnp.exp(final - c))))
        qd.append(queries[g] * grow)
        last.append(jnp.exp(final))

    def same(size):
        return (row // size) == (col // size)

    small = 16
    power = [split(jnp.where(same(small), -lower[h], 0.0)) for h in hs]
    inverse = [eye + jnp.where(same(small), -lower[h], 0.0) for h in hs]
    steps = 1
    while 2**steps < small:
        power = [split(mm(power[h], power[h])) for h in hs]
        inverse = [inverse[h] + mm(split(inverse[h]), power[h]) for h in hs]
        steps += 1
    size = small
    while size < BLOCK:
        between = same(2 * size) & (~same(size))
        cross = [split(jnp.where(between, lower[h], 0.0)) for h in hs]
        parts = [split(inverse[h]) for h in hs]
        mixed = [split(mm(cross[h], parts[h])) for h in hs]
        inverse = [inverse[h] - mm(parts[h], mixed[h]) for h in hs]
        size *= 2
    solved = [split(mm(split(inverse[h]), rhs[h])) for h in hs]
    outs = [mm(scores[h], solved[h]) for h in hs]
    ends = [mm(kdt[h], solved[h]) for h in hs]
    states = [split(st_ref[h]) for h in hs]
    readers = [split(qd[h] - outs[h][:, HEAD_DIM:]) for h in hs]
    maps = [split(last[h] * eye - ends[h][:, HEAD_DIM:]) for h in hs]
    for h in hs:
        seen = mm(readers[h], states[h])
        o_ref[h] = seen[:, :HEAD_DIM] + outs[h][:, :HEAD_DIM]
        m_ref[h] = seen[:, HEAD_DIM:]
    for h in hs:
        moved = mm(maps[h], states[h])
        new = jnp.concatenate([moved[:, :HEAD_DIM] + ends[h][:, :HEAD_DIM], moved[:, HEAD_DIM:]], axis=1)
        st_ref[h] = new
        end_ref[h] = new


def local_terms(heads, meta, q, k, v, g, tail, weights, rates):
    count = q.shape[0] // 2
    seq = count * BLOCK

    def whole(x):
        return pl.BlockSpec(x.shape, lambda b, m, nd=x.ndim: (0,) * nd)

    def per_block():
        return pl.BlockSpec((heads, BLOCK, HEAD_DIM), lambda b, m: (0, b, 0))

    dots = 40 * heads * count
    return pl.pallas_call(
        functools.partial(local_kernel, heads),
        grid_spec=pltpu.PrefetchScalarGridSpec(
            num_scalar_prefetch=1,
            grid=(count,),
            in_specs=[whole(x) for x in (q, k, v, g, tail, weights, rates)],
            out_specs=[
                per_block(),
                per_block(),
                pl.BlockSpec((heads, HEAD_DIM, 2 * HEAD_DIM), lambda b, m: (0, 0, 0)),
            ],
            scratch_shapes=[
                pltpu.VMEM((BLOCK + 8, weights.shape[1]), f32),
                pltpu.VMEM((heads, HEAD_DIM, 2 * HEAD_DIM), f32),
            ],
        ),
        out_shape=(
            jax.ShapeDtypeStruct((heads, seq, HEAD_DIM), f32),
            jax.ShapeDtypeStruct((heads, seq, HEAD_DIM), f32),
            jax.ShapeDtypeStruct((heads, HEAD_DIM, 2 * HEAD_DIM), f32),
        ),
        compiler_params=pltpu.CompilerParams(
            dimension_semantics=("arbitrary",), vmem_limit_bytes=60 * 1024 * 1024
        ),
        cost_estimate=pl.CostEstimate(
            flops=6 * dots * BLOCK**3, bytes_accessed=12 * seq * heads * HEAD_DIM, transcendentals=0
        ),
        name="local_terms",
    )(meta, q, k, v, g, tail, weights, rates)


def chain_kernel(segs, heads, end_ref, inc_ref, out_ref, send, recv):
    seg = lax.axis_index("seg")
    me = lax.axis_index("cp")
    barrier = pltpu.get_barrier_semaphore()

    @pl.when(seg > 0)
    def _():
        pl.semaphore_signal(barrier, inc=1, device_id=(seg - 1, me), device_id_type=MESH)

    @pl.when(seg < segs - 1)
    def _():
        pl.semaphore_wait(barrier, 1)

    def hop(h):
        return pltpu.make_async_remote_copy(
            src_ref=out_ref.at[h],
            dst_ref=inc_ref.at[h],
            send_sem=send.at[h],
            recv_sem=recv.at[h],
            device_id=(lax.rem(seg + 1, segs), me),
            device_id_type=MESH,
        )

    for h in range(heads):
        @pl.when(seg == 0)
        def _():
            inc_ref[h] = jnp.zeros((HEAD_DIM, HEAD_DIM), f32)
            out_ref[h] = end_ref[h, :, :HEAD_DIM]

        @pl.when(seg > 0)
        def _():
            hop(h).wait_recv()

            @pl.when(seg < segs - 1)
            def _():
                out_ref[h] = end_ref[h, :, :HEAD_DIM] + mm(
                    split(end_ref[h, :, HEAD_DIM:]), split(inc_ref[h])
                )

        @pl.when(seg < segs - 1)
        def _():
            hop(h).start()

    for h in range(heads):
        @pl.when(seg < segs - 1)
        def _():
            hop(h).wait_send()


def chain(segs, heads, ends):
    return pl.pallas_call(
        functools.partial(chain_kernel, segs, heads),
        out_shape=jax.ShapeDtypeStruct((heads, HEAD_DIM, HEAD_DIM), f32),
        in_specs=[pl.BlockSpec(memory_space=pltpu.VMEM)],
        out_specs=pl.BlockSpec(memory_space=pltpu.VMEM),
        scratch_shapes=[
            pltpu.VMEM((heads, HEAD_DIM, HEAD_DIM), f32),
            pltpu.SemaphoreType.DMA((heads,)),
            pltpu.SemaphoreType.DMA((heads,)),
        ],
        compiler_params=pltpu.CompilerParams(collective_id=1, has_side_effects=True),
        name="chain",
    )(ends)


def finish_kernel(heads, meta, o_ref, m_ref, inc_ref, z_ref, gain_ref, y_ref):
    b = pl.program_id(0)
    i0 = meta[2 * b]
    i1 = meta[2 * b + 1]
    for h in range(heads):
        cols = slice(h * HEAD_DIM, (h + 1) * HEAD_DIM)
        core = o_ref[h] + mm(split(m_ref[h]), split(inc_ref[h]))
        z = jnp.concatenate([z_ref[i0, :, cols], z_ref[i1, :, cols]], axis=0).astype(f32)
        scale = lax.rsqrt(jnp.sum(core * core, axis=-1, keepdims=True) * (1.0 / HEAD_DIM) + 1e-06)
        y_ref[:, cols] = (core * scale * gain_ref[0:1, :] * (z / (1.0 + jnp.exp(-z)))).astype(bf16)


def finish(heads, meta, local_out, reach, incoming, z, gain):
    count = z.shape[0] // 2
    per_block = pl.BlockSpec((heads, BLOCK, HEAD_DIM), lambda b, m: (0, b, 0))
    return pl.pallas_call(
        functools.partial(finish_kernel, heads),
        grid_spec=pltpu.PrefetchScalarGridSpec(
            num_scalar_prefetch=1,
            grid=(count,),
            in_specs=[
                per_block,
                per_block,
                pl.BlockSpec(incoming.shape, lambda b, m: (0, 0, 0)),
                pl.BlockSpec(z.shape, lambda b, m: (0, 0, 0)),
                pl.BlockSpec(gain.shape, lambda b, m: (0, 0)),
            ],
            out_specs=pl.BlockSpec((BLOCK, heads * HEAD_DIM), lambda b, m: (b, 0)),
        ),
        out_shape=jax.ShapeDtypeStruct((count * BLOCK, heads * HEAD_DIM), bf16),
        compiler_params=pltpu.CompilerParams(dimension_semantics=("arbitrary",)),
        name="finish",
    )(meta, local_out, reach, incoming, z, gain)


def gather_kernel(n, y, out, send, recv, local):
    me = lax.axis_index("cp")
    seg = lax.axis_index("seg")
    rows = y.shape[0] // n
    width = y.shape[1]
    barrier = pltpu.get_barrier_semaphore()
    for d in range(1, n):
        pl.semaphore_signal(
            barrier, inc=1, device_id=(seg, lax.rem(me + d, n)), device_id_type=MESH
        )
    pl.semaphore_wait(barrier, n - 1)

    def src(p):
        return y.at[pl.ds(pl.multiple_of(p * rows, rows), rows), :]

    def dst(p):
        return out.at[:, pl.ds(pl.multiple_of(p * width, width), width)]

    started = []
    for d in range(1, n):
        peer = lax.rem(me + d, n)
        copy = pltpu.make_async_remote_copy(
            src_ref=src(peer),
            dst_ref=dst(me),
            send_sem=send.at[peer],
            recv_sem=recv.at[me],
            device_id=(seg, peer),
            device_id_type=MESH,
        )
        copy.start()
        started.append(copy)
    own = pltpu.make_async_copy(src(me), dst(me), local)
    own.start()
    own.wait()
    for d in range(1, n):
        source = lax.rem(me + n - d, n)
        pltpu.make_async_remote_copy(
            src_ref=src(me),
            dst_ref=dst(source),
            send_sem=send.at[source],
            recv_sem=recv.at[source],
            device_id=(seg, source),
            device_id_type=MESH,
        ).wait_recv()
    for copy in started:
        copy.wait_send()


def gather(n, y):
    return pl.pallas_call(
        functools.partial(gather_kernel, n),
        out_shape=jax.ShapeDtypeStruct((y.shape[0] // n, y.shape[1] * n), y.dtype),
        in_specs=[pl.BlockSpec(memory_space=pltpu.VMEM)],
        out_specs=pl.BlockSpec(memory_space=pltpu.VMEM),
        scratch_shapes=[
            pltpu.SemaphoreType.DMA((n,)),
            pltpu.SemaphoreType.DMA((n,)),
            pltpu.SemaphoreType.DMA,
        ],
        compiler_params=pltpu.CompilerParams(collective_id=2, has_side_effects=True),
        name="gather",
    )(y)


def per_device(mixed_qkv, gate_z, gate_logits, block_table, conv_weight, a_log, dt_bias, norm_gain):
    n = lax.axis_size("cp")
    segs = lax.axis_size("seg")
    me = lax.axis_index("cp")
    seg = lax.axis_index("seg")
    heads = VALUE_HEADS // n
    keys = max(1, heads // GROUP)
    wk, wv = keys * HEAD_DIM, heads * HEAD_DIM
    key_width = KEY_HEADS * HEAD_DIM
    blocks = 2 * n

    prior_table = lax.ppermute(block_table, "seg", [(i, (i + 1) % segs) for i in range(segs)])
    places = jnp.arange(blocks, dtype=jnp.int32)
    order = jnp.sum(
        jnp.where(block_table[0][None, :] == places[:, None], places[None, :], 0), axis=1, dtype=jnp.int32
    )
    tail_from = jnp.sum(jnp.where(prior_table[0] == blocks - 1, places, 0), dtype=jnp.int32) // 2
    meta = jnp.concatenate(
        [order, jnp.stack([tail_from, (seg == 0).astype(jnp.int32), (me * heads).astype(jnp.int32)])]
    )
    kcol = me * heads // GROUP * HEAD_DIM
    weights = jnp.concatenate(
        [
            lax.dynamic_slice_in_dim(conv_weight, kcol, wk, 1),
            lax.dynamic_slice_in_dim(conv_weight, key_width + kcol, wk, 1),
            lax.dynamic_slice_in_dim(conv_weight, 2 * key_width + me * wv, wv, 1),
        ],
        axis=1,
    )
    spare = HEAD_DIM - 2 * VALUE_HEADS
    rates = jnp.stack(
        [jnp.pad(-jnp.exp(a_log), (VALUE_HEADS, spare)), jnp.pad(dt_bias, (VALUE_HEADS, spare))]
    )
    q, k, v, z, g, tail = scatter(n, segs, heads, mixed_qkv, gate_z, gate_logits)

    def stored(x):
        return x.reshape(blocks, x.shape[1] // 2, x.shape[2])

    local_out, reach, ends = local_terms(
        heads, meta, stored(q), stored(k), stored(v), stored(g), tail, weights, rates
    )
    incoming = chain(segs, heads, ends)
    y = finish(heads, meta, local_out, reach, incoming, stored(z), norm_gain[None, :])
    return gather(n, y)


def solution(mesh):
    return jax.shard_map(
        per_device,
        mesh=mesh,
        in_specs=(
            P(("seg", "cp"), None),
            P(("seg", "cp"), None),
            P(("seg", "cp"), None),
            P("seg", None),
            P(),
            P(),
            P(),
            P(),
        ),
        out_specs=P(("seg", "cp"), None),
        check_vma=False,
    )
```

```python
import functools

import jax
import jax.numpy as jnp
from jax import lax
from jax.experimental import pallas as pl
from jax.experimental.pallas import tpu as pltpu
from jax.sharding import PartitionSpec as P

VALUE_HEADS = 32
KEY_HEADS = 16
HEAD_DIM = 128
CONV = 4
BLOCK = 128
TAIL = 8
GROUP = VALUE_HEADS // KEY_HEADS

f32 = jnp.float32
bf16 = jnp.bfloat16
MESH = pl.DeviceIdType.MESH
highest = lax.Precision.HIGHEST


def split(x):
    hi = x.astype(bf16)
    return hi, (x - hi.astype(f32)).astype(bf16)


NN = (((1,), (0,)), ((), ()))
NT = (((1,), (1,)), ((), ()))


def mm(a, b, dims=NN):
    def dot(x, y):
        return lax.dot_general(x, y, dims, preferred_element_type=f32)

    return dot(a[0], b[0]) + (dot(a[0], b[1]) + dot(a[1], b[0]))


def log1p_exact(y):
    u = 1.0 + y
    return jnp.where(u == 1.0, y, jnp.log(u) * (y / jnp.where(u == 1.0, 1.0, u - 1.0)))


def block_step(
    heads, b, start, order, parts_now, first_prior, head_start, w_ref, rate_ref, o_ref, mh_ref, ml_ref, st_ref, x_ref
):
    keys = max(1, heads // GROUP)
    wk, wv = keys * HEAD_DIM, heads * HEAD_DIM
    i0 = order[2 * b] // 2
    i1 = order[2 * b + 1] // 2
    ip = order[jnp.maximum(2 * b - 1, 0)] // 2
    half = parts_now[0].shape[1]

    row = lax.broadcasted_iota(jnp.int32, (BLOCK, BLOCK), 0)
    col = lax.broadcasted_iota(jnp.int32, (BLOCK, BLOCK), 1)
    strict = row > col
    inclusive = row >= col
    eye = jnp.where(row == col, 1.0, 0.0).astype(f32)

    at = 0
    for place, width in enumerate((wk, wk, wv)):
        cols = slice(at, at + width)
        ref = parts_now[place]
        prior = ref[ip, half - 16 :, :].astype(f32)[8:]
        x_ref[0:8, cols] = jnp.where(b == start, first_prior(place, cols), prior)
        x_ref[8 : 8 + half, cols] = ref[i0].astype(f32)
        x_ref[8 + half : 8 + 2 * half, cols] = ref[i1].astype(f32)
        at += width

    def conv(start):
        cols = slice(start, start + HEAD_DIM)
        total_rows = w_ref[0:1, cols] * x_ref[5 : 5 + BLOCK, cols]
        for j in range(1, CONV):
            total_rows = total_rows + w_ref[j : j + 1, cols] * x_ref[5 + j : 5 + j + BLOCK, cols]
        return total_rows / (1.0 + jnp.exp(-total_rows))

    def unit(x):
        return x * lax.rsqrt(jnp.sum(x * x, axis=-1, keepdims=True) + 1e-06)

    gates = jnp.concatenate([parts_now[3][i0], parts_now[3][i1]], axis=0).astype(f32)
    gates = jnp.concatenate([gates, jnp.zeros((BLOCK, BLOCK - gates.shape[1]), f32)], axis=1)
    beta_all = 1.0 / (1.0 + jnp.exp(-gates))
    shifted = gates + rate_ref[1:2, :]
    soft = jnp.maximum(shifted, 0.0) + log1p_exact(jnp.exp(-jnp.abs(shifted)))
    decays = rate_ref[0:1, :] * soft
    turn = lax.rem(BLOCK - head_start, BLOCK)
    beta_all = pltpu.roll(beta_all, turn, 1)
    decays = pltpu.roll(decays, turn, 1)
    tril = jnp.where(inclusive, 1.0, 0.0).astype(bf16)
    d0 = decays.astype(bf16)
    rest = decays - d0.astype(f32)
    d1 = rest.astype(bf16)
    d2 = (rest - d1.astype(f32)).astype(bf16)
    cum = jnp.dot(tril, d2, preferred_element_type=f32)
    cum = cum + jnp.dot(tril, d1, preferred_element_type=f32)
    cum = cum + jnp.dot(tril, d0, preferred_element_type=f32)
    cum_t = jnp.transpose(cum)

    queries, key_rows, kk, qk = [], [], [], []
    for g in range(keys):
        queries.append(unit(conv(g * HEAD_DIM)) * HEAD_DIM ** (-0.5))
        key_rows.append(unit(conv(wk + g * HEAD_DIM)))
        ks = split(key_rows[g])
        qs = split(queries[g])
        kk.append(mm(ks, ks, NT))
        qk.append(mm(qs, ks, NT))

    hs = range(heads)
    lower, scores, rhs, kdt, qd, last = [], [], [], [], [], []
    for h in hs:
        g = h * keys // heads
        beta = beta_all[:, h : h + 1]
        c = cum[:, VALUE_HEADS + h : VALUE_HEADS + h + 1]
        ct = cum_t[VALUE_HEADS + h : VALUE_HEADS + h + 1, :]
        final = ct[:, BLOCK - 1 :]
        spread = c - ct
        incl = jnp.where(inclusive, jnp.exp(jnp.where(inclusive, spread, 0.0)), 0.0)
        lower.append(jnp.where(strict, beta * kk[g] * incl, 0.0))
        scores.append(split(qk[g] * incl))
        grow = jnp.exp(c)
        values = conv(2 * wk + h * HEAD_DIM)
        rhs.append(split(jnp.concatenate([values * beta, key_rows[g] * (beta * grow)], axis=1)))
        kdt.append(split(jnp.transpose(key_rows[g] * jnp.exp(final - c))))
        qd.append(queries[g] * grow)
        last.append(jnp.exp(final))

    def same(size):
        return (row // size) == (col // size)

    small = 16
    power = [split(jnp.where(same(small), -lower[h], 0.0)) for h in hs]
    inverse = [eye + jnp.where(same(small), -lower[h], 0.0) for h in hs]
    steps = 1
    while 2**steps < small:
        power = [split(mm(power[h], power[h])) for h in hs]
        inverse = [inverse[h] + mm(split(inverse[h]), power[h]) for h in hs]
        steps += 1
    size = small
    while size < BLOCK:
        between = same(2 * size) & (~same(size))
        cross = [split(jnp.where(between, lower[h], 0.0)) for h in hs]
        parts = [split(inverse[h]) for h in hs]
        mixed = [split(mm(cross[h], parts[h])) for h in hs]
        inverse = [inverse[h] - mm(parts[h], mixed[h]) for h in hs]
        size *= 2
    solved = [split(mm(split(inverse[h]), rhs[h])) for h in hs]
    outs = [mm(scores[h], solved[h]) for h in hs]
    ends = [mm(kdt[h], solved[h]) for h in hs]
    states = [split(st_ref[h]) for h in hs]
    readers = [split(qd[h] - outs[h][:, HEAD_DIM:]) for h in hs]
    maps = [split(last[h] * eye - ends[h][:, HEAD_DIM:]) for h in hs]
    for h in hs:
        seen = mm(readers[h], states[h])
        o_ref[h, b] = seen[:, :HEAD_DIM] + outs[h][:, :HEAD_DIM]
        reach = split(seen[:, HEAD_DIM:])
        mh_ref[h, b] = reach[0]
        ml_ref[h, b] = reach[1]
    for h in hs:
        moved = mm(maps[h], states[h])
        new = jnp.concatenate([moved[:, :HEAD_DIM] + ends[h][:, :HEAD_DIM], moved[:, HEAD_DIM:]], axis=1)
        st_ref[h] = new


def mix_kernel(
    n, segs, heads, order, qkv, z, gates, conv_weight, rate_ref, o_ref, mh_ref, ml_ref, st_ref, oz,
    qa, ka, va, ga, qb, kb, vb, gb, otail, w_ref, x_ref, send, recv, local
):
    me = lax.axis_index("cp")
    seg = lax.axis_index("seg")
    after = lax.rem(seg + 1, segs)
    before = lax.rem(seg + segs - 1, segs)
    keys = max(1, heads // GROUP)
    wk, wv = keys * HEAD_DIM, heads * HEAD_DIM
    key_width = KEY_HEADS * HEAD_DIM
    rows = qkv.shape[0]
    half = rows // 2

    barrier = pltpu.get_barrier_semaphore()
    for d in range(n):
        peer = lax.rem(me + d, n)
        if d:
            pl.semaphore_signal(barrier, inc=1, device_id=(seg, peer), device_id_type=MESH)
        pl.semaphore_signal(barrier, inc=1, device_id=(before, peer), device_id_type=MESH)

    def columns(start, width):
        return pl.ds(pl.multiple_of(start, HEAD_DIM), width)

    def pieces(p, slot):
        kcol = lax.div(p * heads, GROUP) * HEAD_DIM
        vcol = p * wv
        found = []
        for first, bufs in ((0, (qa, ka, va, ga)), (half, (qb, kb, vb, gb))):
            these = pl.ds(first, half)
            found += [
                (qkv.at[these, columns(kcol, wk)], bufs[0].at[slot]),
                (qkv.at[these, columns(key_width + kcol, wk)], bufs[1].at[slot]),
                (qkv.at[these, columns(2 * key_width + vcol, wv)], bufs[2].at[slot]),
                (gates.at[these], bufs[3].at[slot]),
            ]
        return found + [(z.at[:, columns(vcol, wv)], oz.at[slot])]

    def tails(p, slot):
        kcol = lax.div(p * heads, GROUP) * HEAD_DIM
        vcol = p * wv
        last = pl.ds(rows - TAIL, TAIL)
        return [
            (qkv.at[last, columns(kcol, wk)], otail.at[slot, :, pl.ds(0, wk)]),
            (qkv.at[last, columns(key_width + kcol, wk)], otail.at[slot, :, pl.ds(wk, wk)]),
            (qkv.at[last, columns(2 * key_width + vcol, wv)], otail.at[slot, :, pl.ds(2 * wk, wv)]),
        ]

    own = []
    kcol = lax.div(me * heads, GROUP) * HEAD_DIM
    mine = pieces(me, me) + [
        (conv_weight.at[:, columns(kcol, wk)], w_ref.at[:, pl.ds(0, wk)]),
        (conv_weight.at[:, columns(key_width + kcol, wk)], w_ref.at[:, pl.ds(wk, wk)]),
        (conv_weight.at[:, columns(2 * key_width + me * wv, wv)], w_ref.at[:, pl.ds(2 * wk, wv)]),
    ]
    for kind, (src, dst) in enumerate(mine):
        copy = pltpu.make_async_copy(src, dst, local.at[kind])
        copy.start()
        own.append(copy)
    pl.semaphore_wait(barrier, 2 * n - 1)

    started = []

    def post(kind, src, dst, peer, target):
        copy = pltpu.make_async_remote_copy(
            src_ref=src,
            dst_ref=dst,
            send_sem=send.at[kind, peer],
            recv_sem=recv.at[kind, me],
            device_id=target,
            device_id_type=MESH,
        )
        copy.start()
        started.append(copy)

    for kinds in ((0, 1, 2, 3), (4, 5, 6, 7), (8,)):
        for d in range(1, n):
            peer = lax.rem(me + d, n)
            sources = pieces(peer, me)
            for kind in kinds:
                post(kind, *sources[kind], peer, (seg, peer))
        if kinds[0] == 0:
            for d in range(n):
                peer = lax.rem(me + d, n)
                for i, (src, dst) in enumerate(tails(peer, me)):
                    post(9 + i, src, dst, peer, (after, peer))

    def arrived(kinds):
        for d in range(n):
            source = lax.rem(me + n - d, n)
            found = pieces(me, source) + tails(me, source)
            for kind in kinds:
                if d or kind > 8:
                    src, dst = found[kind]
                    pltpu.make_async_remote_copy(
                        src_ref=src,
                        dst_ref=dst,
                        send_sem=send.at[kind, source],
                        recv_sem=recv.at[kind, source],
                        device_id=(seg, source),
                        device_id_type=MESH,
                    ).wait_recv()

    row = lax.broadcasted_iota(jnp.int32, (HEAD_DIM, HEAD_DIM), 0)
    col = lax.broadcasted_iota(jnp.int32, (HEAD_DIM, HEAD_DIM), 1)
    for h in range(heads):
        st_ref[h, :, :HEAD_DIM] = jnp.zeros((HEAD_DIM, HEAD_DIM), f32)
        st_ref[h, :, HEAD_DIM:] = jnp.where(row == col, 1.0, 0.0).astype(f32)
    for copy in own:
        copy.wait()
    tail_from = order[2 * n]
    joint = order[n - 1] // 2
    early = (qa, ka, va, ga)
    late = (qb, kb, vb, gb)

    def from_tail(place, cols):
        return jnp.where(seg == 0, 0.0, otail[tail_from].astype(f32)[:, cols])

    def from_early(place, cols):
        return early[place][joint, half - 16 :, :].astype(f32)[8:]

    def run(first, stop, bufs, prior):
        def one(b, carry):
            block_step(
                heads, b, first, order, bufs, prior, me * heads,
                w_ref, rate_ref, o_ref, mh_ref, ml_ref, st_ref, x_ref,
            )
            return carry

        lax.fori_loop(first, stop, one, 0)

    arrived((0, 1, 2, 3, 9, 10, 11))
    run(0, n // 2, early, from_tail)
    arrived((4, 5, 6, 7))
    run(n // 2, n, late, from_early)
    arrived((8,))
    for copy in started:
        copy.wait_send()


def mix(n, segs, heads, order, qkv, z, gates, conv_weight, rates):
    keys = max(1, heads // GROUP)
    wk, wv = keys * HEAD_DIM, heads * HEAD_DIM
    rows = qkv.shape[0]
    half = rows // 2
    anywhere = pl.BlockSpec(memory_space=pl.ANY)
    vmem = pl.BlockSpec(memory_space=pltpu.VMEM)
    widths = (wk, wk, wv, gates.shape[1])
    return pl.pallas_call(
        functools.partial(mix_kernel, n, segs, heads),
        out_shape=(
            jax.ShapeDtypeStruct((heads, n, BLOCK, HEAD_DIM), f32),
            jax.ShapeDtypeStruct((heads, n, BLOCK, HEAD_DIM), bf16),
            jax.ShapeDtypeStruct((heads, n, BLOCK, HEAD_DIM), bf16),
            jax.ShapeDtypeStruct((heads, HEAD_DIM, 2 * HEAD_DIM), f32),
            jax.ShapeDtypeStruct((n, rows, wv), bf16),
        ),
        in_specs=[pl.BlockSpec(memory_space=pltpu.SMEM)] + [anywhere] * 4 + [vmem],
        out_specs=[vmem] * 5,
        scratch_shapes=[pltpu.VMEM((n, half, w), bf16) for w in widths]
        + [pltpu.VMEM((n, half, w), bf16) for w in widths]
        + [
            pltpu.VMEM((n, TAIL, 2 * wk + wv), bf16),
            pltpu.VMEM((CONV, 2 * wk + wv), f32),
            pltpu.VMEM((BLOCK + 8, 2 * wk + wv), f32),
            pltpu.SemaphoreType.DMA((12, n)),
            pltpu.SemaphoreType.DMA((12, n)),
            pltpu.SemaphoreType.DMA((12,)),
        ],
        compiler_params=pltpu.CompilerParams(
            collective_id=0, has_side_effects=True, vmem_limit_bytes=40 * 1024 * 1024
        ),
        name="mix",
    )(order, qkv, z, gates, conv_weight, rates)


def close_kernel(
    n, segs, heads, order, end_ref, o_ref, mh_ref, ml_ref, z_ref, gain_ref, out,
    inc_ref, pass_ref, y_ref, send, recv, ysend, yrecv, local
):
    seg = lax.axis_index("seg")
    me = lax.axis_index("cp")
    final = segs - 1
    width = heads * HEAD_DIM
    barrier = pltpu.get_barrier_semaphore()
    for d in range(1, n):
        pl.semaphore_signal(
            barrier, inc=1, device_id=(seg, lax.rem(me + d, n)), device_id_type=MESH
        )
    pl.semaphore_signal(
        barrier, inc=1, device_id=(lax.rem(seg + segs - 1, segs), me), device_id_type=MESH
    )
    pl.semaphore_wait(barrier, n)

    def hop(h):
        return pltpu.make_async_remote_copy(
            src_ref=pass_ref.at[h],
            dst_ref=inc_ref.at[h],
            send_sem=send.at[h],
            recv_sem=recv.at[h],
            device_id=(lax.rem(seg + 1, segs), me),
            device_id_type=MESH,
        )

    @pl.when(seg == 0)
    def _():
        for h in range(heads):
            inc_ref[h] = jnp.zeros((HEAD_DIM, HEAD_DIM), f32)
            pass_ref[h] = end_ref[h, :, :HEAD_DIM]
        for h in range(heads):
            hop(h).start()

    @pl.when((seg > 0) & (seg < final))
    def _():
        for h in range(heads):
            through = split(end_ref[h, :, HEAD_DIM:])
            hop(h).wait_recv()
            pass_ref[h] = end_ref[h, :, :HEAD_DIM] + mm(through, split(inc_ref[h]))
            hop(h).start()

    def block(h, b, state):
        cols = pl.ds(h * HEAD_DIM, HEAD_DIM)
        i0 = order[2 * b]
        i1 = order[2 * b + 1]
        core = o_ref[h, b] + mm((mh_ref[h, b], ml_ref[h, b]), state)
        z = jnp.concatenate([z_ref[i0, :, cols], z_ref[i1, :, cols]], axis=0).astype(f32)
        scale = lax.rsqrt(jnp.sum(core * core, axis=-1, keepdims=True) * (1.0 / HEAD_DIM) + 1e-06)
        y_ref[h, b] = (core * scale * gain_ref[0:1, :] * (z / (1.0 + jnp.exp(-z)))).astype(bf16)

    def target(h, source):
        return out.at[:, pl.ds(pl.multiple_of(source * width + h * HEAD_DIM, HEAD_DIM), HEAD_DIM)]

    def give(h, d):
        peer = lax.rem(me + d, n)
        return pltpu.make_async_remote_copy(
            src_ref=y_ref.at[h, peer],
            dst_ref=target(h, me),
            send_sem=ysend.at[h, peer],
            recv_sem=yrecv.at[h, me],
            device_id=(seg, peer),
            device_id_type=MESH,
        )

    for h in range(heads):
        @pl.when(seg == final)
        def _():
            hop(h).wait_recv()

        state = split(inc_ref[h])

        for d in range(1, n):
            block(h, lax.rem(me + d, n), state)
            if d > 1:
                give(h, d - 1).start()
        block(h, me, state)
        give(h, n - 1).start()
        if h:
            pltpu.make_async_copy(y_ref.at[h - 1, me], target(h - 1, me), local.at[h - 1]).start()
    pltpu.make_async_copy(y_ref.at[heads - 1, me], target(heads - 1, me), local.at[heads - 1]).start()

    for h in range(heads):
        pltpu.make_async_copy(y_ref.at[h, me], target(h, me), local.at[h]).wait()
        for d in range(1, n):
            source = lax.rem(me + n - d, n)
            pltpu.make_async_remote_copy(
                src_ref=y_ref.at[h, source],
                dst_ref=target(h, source),
                send_sem=ysend.at[h, source],
                recv_sem=yrecv.at[h, source],
                device_id=(seg, source),
                device_id_type=MESH,
            ).wait_recv()
    for h in range(heads):
        for d in range(1, n):
            give(h, d).wait_send()

        @pl.when(seg < final)
        def _():
            hop(h).wait_send()


def close(n, segs, heads, order, ends, o, mh, ml, z, gain):
    vmem = pl.BlockSpec(memory_space=pltpu.VMEM)
    return pl.pallas_call(
        functools.partial(close_kernel, n, segs, heads),
        out_shape=jax.ShapeDtypeStruct((BLOCK, n * heads * HEAD_DIM), bf16),
        in_specs=[pl.BlockSpec(memory_space=pltpu.SMEM)] + [vmem] * 6,
        out_specs=vmem,
        scratch_shapes=[
            pltpu.VMEM((heads, HEAD_DIM, HEAD_DIM), f32),
            pltpu.VMEM((heads, HEAD_DIM, HEAD_DIM), f32),
            pltpu.VMEM((heads, n, BLOCK, HEAD_DIM), bf16),
            pltpu.SemaphoreType.DMA((heads,)),
            pltpu.SemaphoreType.DMA((heads,)),
            pltpu.SemaphoreType.DMA((heads, n)),
            pltpu.SemaphoreType.DMA((heads, n)),
            pltpu.SemaphoreType.DMA((heads,)),
        ],
        compiler_params=pltpu.CompilerParams(
            collective_id=1, has_side_effects=True, vmem_limit_bytes=40 * 1024 * 1024
        ),
        name="close",
    )(order, ends, o, mh, ml, z, gain)


def per_device(mixed_qkv, gate_z, gate_logits, block_table, conv_weight, a_log, dt_bias, norm_gain):
    n = lax.axis_size("cp")
    segs = lax.axis_size("seg")
    heads = VALUE_HEADS // n
    blocks = 2 * n

    prior_table = lax.ppermute(block_table, "seg", [(i, (i + 1) % segs) for i in range(segs)])
    places = jnp.arange(blocks, dtype=jnp.int32)
    order = jnp.sum(
        jnp.where(block_table[0][None, :] == places[:, None], places[None, :], 0), axis=1, dtype=jnp.int32
    )
    tail_from = jnp.sum(jnp.where(prior_table[0] == blocks - 1, places, 0), dtype=jnp.int32) // 2
    order = jnp.concatenate([order, tail_from[None]])
    spare = HEAD_DIM - 2 * VALUE_HEADS
    rates = jnp.stack(
        [jnp.pad(-jnp.exp(a_log), (VALUE_HEADS, spare)), jnp.pad(dt_bias, (VALUE_HEADS, spare))]
    )
    o, mh, ml, ends, z = mix(
        n, segs, heads, order, mixed_qkv, gate_z, gate_logits, conv_weight, rates
    )
    z = z.reshape(blocks, z.shape[1] // 2, z.shape[2])
    return close(n, segs, heads, order, ends, o, mh, ml, z, norm_gain[None, :])


def solution(mesh):
    return jax.shard_map(
        per_device,
        mesh=mesh,
        in_specs=(
            P(("seg", "cp"), None),
            P(("seg", "cp"), None),
            P(("seg", "cp"), None),
            P("seg", None),
            P(),
            P(),
            P(),
            P(),
        ),
        out_specs=P(("seg", "cp"), None),
        check_vma=False,
    )
```

```python
import functools

import jax
import jax.numpy as jnp
from jax import lax
from jax.experimental import pallas as pl
from jax.experimental.pallas import tpu as pltpu
from jax.sharding import PartitionSpec as P

VALUE_HEADS = 32
KEY_HEADS = 16
HEAD_DIM = 128
CONV = 4
BLOCK = 128
TAIL = 8
GROUP = VALUE_HEADS // KEY_HEADS
PAIR = 2

f32 = jnp.float32
bf16 = jnp.bfloat16
MESH = pl.DeviceIdType.MESH
highest = lax.Precision.HIGHEST


def split(x):
    hi = x.astype(bf16)
    return hi, (x - hi.astype(f32)).astype(bf16)


NN = (((1,), (0,)), ((), ()))
NT = (((1,), (1,)), ((), ()))


def mm(a, b, dims=NN):
    def dot(x, y):
        return lax.dot_general(x, y, dims, preferred_element_type=f32)

    if dims == NT:
        return dot(a[0], b[0]) + (dot(a[0], b[1]) + dot(a[1], b[0]))
    wide = jnp.concatenate(a, axis=1)
    if b[0].shape[1] > HEAD_DIM:
        return dot(wide, jnp.concatenate([b[0], b[0]], axis=0)) + dot(a[0], b[1])
    top = jnp.concatenate([b[0], b[1]], axis=1)
    low = jnp.concatenate([b[0], jnp.zeros_like(b[1])], axis=1)
    both = dot(wide, jnp.concatenate([top, low], axis=0))
    return both[:, :HEAD_DIM] + both[:, HEAD_DIM:]


def log1p_exact(y):
    u = 1.0 + y
    return jnp.where(u == 1.0, y, jnp.log(u) * (y / jnp.where(u == 1.0, 1.0, u - 1.0)))


def prepare(
    heads, b, start, order, parts_now, first_prior, head_start, w_ref, rate_ref, x_ref
):
    keys = max(1, heads // GROUP)
    wk, wv = keys * HEAD_DIM, heads * HEAD_DIM
    i0 = order[2 * b] // 2
    i1 = order[2 * b + 1] // 2
    ip = order[jnp.maximum(2 * b - 1, 0)] // 2
    half = parts_now[0].shape[1]

    row = lax.broadcasted_iota(jnp.int32, (BLOCK, BLOCK), 0)
    col = lax.broadcasted_iota(jnp.int32, (BLOCK, BLOCK), 1)
    strict = row > col
    inclusive = row >= col
    eye = jnp.where(row == col, 1.0, 0.0).astype(f32)

    at = 0
    for place, width in enumerate((wk, wk, wv)):
        cols = slice(at, at + width)
        ref = parts_now[place]
        prior = ref[ip, half - 16 :, :].astype(f32)[8:]
        x_ref[0:8, cols] = jnp.where(b == start, first_prior(place, cols), prior)
        x_ref[8 : 8 + half, cols] = ref[i0].astype(f32)
        x_ref[8 + half : 8 + 2 * half, cols] = ref[i1].astype(f32)
        at += width

    def conv(start):
        cols = slice(start, start + HEAD_DIM)
        total_rows = w_ref[0:1, cols] * x_ref[5 : 5 + BLOCK, cols]
        for j in range(1, CONV):
            total_rows = total_rows + w_ref[j : j + 1, cols] * x_ref[5 + j : 5 + j + BLOCK, cols]
        return total_rows / (1.0 + jnp.exp(-total_rows))

    def unit(x):
        return x * lax.rsqrt(jnp.sum(x * x, axis=-1, keepdims=True) + 1e-06)

    gates = jnp.concatenate([parts_now[3][i0], parts_now[3][i1]], axis=0).astype(f32)
    gates = jnp.concatenate([gates, jnp.zeros((BLOCK, BLOCK - gates.shape[1]), f32)], axis=1)
    beta_all = 1.0 / (1.0 + jnp.exp(-gates))
    shifted = gates + rate_ref[1:2, :]
    soft = jnp.maximum(shifted, 0.0) + log1p_exact(jnp.exp(-jnp.abs(shifted)))
    decays = rate_ref[0:1, :] * soft
    turn = lax.rem(BLOCK - head_start, BLOCK)
    beta_all = pltpu.roll(beta_all, turn, 1)
    decays = pltpu.roll(decays, turn, 1)
    tril = jnp.where(inclusive, 1.0, 0.0).astype(bf16)
    d0 = decays.astype(bf16)
    rest = decays - d0.astype(f32)
    d1 = rest.astype(bf16)
    d2 = (rest - d1.astype(f32)).astype(bf16)
    cum = jnp.dot(tril, d2, preferred_element_type=f32)
    cum = cum + jnp.dot(tril, d1, preferred_element_type=f32)
    cum = cum + jnp.dot(tril, d0, preferred_element_type=f32)
    cum_t = jnp.transpose(cum)

    queries, key_rows, kk, qk = [], [], [], []
    for g in range(keys):
        queries.append(unit(conv(g * HEAD_DIM)) * HEAD_DIM ** (-0.5))
        key_rows.append(unit(conv(wk + g * HEAD_DIM)))
        ks = split(key_rows[g])
        qs = split(queries[g])
        kk.append(mm(ks, ks, NT))
        qk.append(mm(qs, ks, NT))

    hs = range(heads)
    lower, scores, rhs, kdt, qd, last = [], [], [], [], [], []
    for h in hs:
        g = h * keys // heads
        beta = beta_all[:, h : h + 1]
        c = cum[:, VALUE_HEADS + h : VALUE_HEADS + h + 1]
        ct = cum_t[VALUE_HEADS + h : VALUE_HEADS + h + 1, :]
        final = ct[:, BLOCK - 1 :]
        spread = c - ct
        incl = jnp.where(inclusive, jnp.exp(jnp.where(inclusive, spread, 0.0)), 0.0)
        lower.append(jnp.where(strict, beta * kk[g] * incl, 0.0))
        scores.append(split(qk[g] * incl))
        grow = jnp.exp(c)
        values = conv(2 * wk + h * HEAD_DIM)
        rhs.append(split(jnp.concatenate([values * beta, key_rows[g] * (beta * grow)], axis=1)))
        kdt.append(split(jnp.transpose(key_rows[g] * jnp.exp(final - c))))
        qd.append(queries[g] * grow)
        last.append(jnp.exp(final))

    return lower, scores, rhs, kdt, qd, last


def block_pair(
    heads, pair, start, order, parts_now, first_prior, head_start, w_ref, rate_ref, o_ref, mh_ref, ml_ref, st_ref, x_ref
):
    row = lax.broadcasted_iota(jnp.int32, (BLOCK, BLOCK), 0)
    col = lax.broadcasted_iota(jnp.int32, (BLOCK, BLOCK), 1)
    eye = jnp.where(row == col, 1.0, 0.0).astype(f32)
    lower, scores, rhs, kdt, qd, last = [], [], [], [], [], []
    for e in range(PAIR):
        found = prepare(
            heads, PAIR * pair + e, start, order, parts_now, first_prior, head_start, w_ref, rate_ref, x_ref.at[e]
        )
        for total, more in zip((lower, scores, rhs, kdt, qd, last), found):
            total += more
    hs = range(PAIR * heads)

    def same(size):
        return (row // size) == (col // size)

    small = 16
    power = [split(jnp.where(same(small), -lower[h], 0.0)) for h in hs]
    inverse = [eye + jnp.where(same(small), -lower[h], 0.0) for h in hs]
    steps = 1
    while 2**steps < small:
        power = [split(mm(power[h], power[h])) for h in hs]
        inverse = [inverse[h] + mm(split(inverse[h]), power[h]) for h in hs]
        steps += 1
    size = small
    while size < BLOCK:
        between = same(2 * size) & (~same(size))
        cross = [split(jnp.where(between, lower[h], 0.0)) for h in hs]
        parts = [split(inverse[h]) for h in hs]
        mixed = [split(mm(cross[h], parts[h])) for h in hs]
        inverse = [inverse[h] - mm(parts[h], mixed[h]) for h in hs]
        size *= 2
    solved = [split(mm(split(inverse[h]), rhs[h])) for h in hs]
    outs = [mm(scores[h], solved[h]) for h in hs]
    ends = [mm(kdt[h], solved[h]) for h in hs]
    readers = [split(qd[h] - outs[h][:, HEAD_DIM:]) for h in hs]
    maps = [split(last[h] * eye - ends[h][:, HEAD_DIM:]) for h in hs]
    for e in range(PAIR):
        b = PAIR * pair + e
        states = [split(st_ref[h]) for h in range(heads)]
        for h in range(heads):
            at = e * heads + h
            moved = mm(maps[at], states[h])
            st_ref[h] = jnp.concatenate(
                [moved[:, :HEAD_DIM] + ends[at][:, :HEAD_DIM], moved[:, HEAD_DIM:]], axis=1
            )
        for h in range(heads):
            at = e * heads + h
            seen = mm(readers[at], states[h])
            o_ref[h, b] = seen[:, :HEAD_DIM] + outs[at][:, :HEAD_DIM]
            reach = split(seen[:, HEAD_DIM:])
            mh_ref[h, b] = reach[0]
            ml_ref[h, b] = reach[1]


def mix_kernel(
    n, segs, heads, order, qkv, z, gates, conv_weight, rate_ref, o_ref, mh_ref, ml_ref, st_ref, oz,
    qa, ka, va, ga, qb, kb, vb, gb, otail, w_ref, x_ref, send, recv, local
):
    me = lax.axis_index("cp")
    seg = lax.axis_index("seg")
    after = lax.rem(seg + 1, segs)
    before = lax.rem(seg + segs - 1, segs)
    keys = max(1, heads // GROUP)
    wk, wv = keys * HEAD_DIM, heads * HEAD_DIM
    key_width = KEY_HEADS * HEAD_DIM
    rows = qkv.shape[0]
    half = rows // 2

    barrier = pltpu.get_barrier_semaphore()
    for d in range(n):
        peer = lax.rem(me + d, n)
        if d:
            pl.semaphore_signal(barrier, inc=1, device_id=(seg, peer), device_id_type=MESH)
        pl.semaphore_signal(barrier, inc=1, device_id=(before, peer), device_id_type=MESH)

    def columns(start, width):
        return pl.ds(pl.multiple_of(start, HEAD_DIM), width)

    def pieces(p, slot):
        kcol = lax.div(p * heads, GROUP) * HEAD_DIM
        vcol = p * wv
        found = []
        for first, bufs in ((0, (qa, ka, va, ga)), (half, (qb, kb, vb, gb))):
            these = pl.ds(first, half)
            found += [
                (qkv.at[these, columns(kcol, wk)], bufs[0].at[slot]),
                (qkv.at[these, columns(key_width + kcol, wk)], bufs[1].at[slot]),
                (qkv.at[these, columns(2 * key_width + vcol, wv)], bufs[2].at[slot]),
                (gates.at[these], bufs[3].at[slot]),
            ]
        return found + [
            (z.at[pl.ds(0, half), columns(vcol, wv)], oz.at[2 * slot]),
            (z.at[pl.ds(half, half), columns(vcol, wv)], oz.at[2 * slot + 1]),
        ]

    def tails(p, slot):
        kcol = lax.div(p * heads, GROUP) * HEAD_DIM
        vcol = p * wv
        last = pl.ds(rows - TAIL, TAIL)
        return [
            (qkv.at[last, columns(kcol, wk)], otail.at[slot, :, pl.ds(0, wk)]),
            (qkv.at[last, columns(key_width + kcol, wk)], otail.at[slot, :, pl.ds(wk, wk)]),
            (qkv.at[last, columns(2 * key_width + vcol, wv)], otail.at[slot, :, pl.ds(2 * wk, wv)]),
        ]

    own = []
    kcol = lax.div(me * heads, GROUP) * HEAD_DIM
    mine = pieces(me, me) + [
        (conv_weight.at[:, columns(kcol, wk)], w_ref.at[:, pl.ds(0, wk)]),
        (conv_weight.at[:, columns(key_width + kcol, wk)], w_ref.at[:, pl.ds(wk, wk)]),
        (conv_weight.at[:, columns(2 * key_width + me * wv, wv)], w_ref.at[:, pl.ds(2 * wk, wv)]),
    ]
    for kind, (src, dst) in enumerate(mine):
        copy = pltpu.make_async_copy(src, dst, local.at[kind])
        copy.start()
        own.append(copy)
    pl.semaphore_wait(barrier, 2 * n - 1)

    started = []

    def post(kind, src, dst, peer, target):
        copy = pltpu.make_async_remote_copy(
            src_ref=src,
            dst_ref=dst,
            send_sem=send.at[kind, peer],
            recv_sem=recv.at[kind, me],
            device_id=target,
            device_id_type=MESH,
        )
        copy.start()
        started.append(copy)

    for kinds in ((0, 1, 2, 3), (4, 5, 6, 7), (8, 9)):
        for d in range(1, n):
            peer = lax.rem(me + d, n)
            sources = pieces(peer, me)
            for kind in kinds:
                post(kind, *sources[kind], peer, (seg, peer))
        if kinds[0] == 0:
            for d in range(n):
                peer = lax.rem(me + d, n)
                for i, (src, dst) in enumerate(tails(peer, me)):
                    post(10 + i, src, dst, peer, (after, peer))

    def arrived(kinds):
        for d in range(n):
            source = lax.rem(me + n - d, n)
            found = pieces(me, source) + tails(me, source)
            for kind in kinds:
                if d or kind > 9:
                    src, dst = found[kind]
                    pltpu.make_async_remote_copy(
                        src_ref=src,
                        dst_ref=dst,
                        send_sem=send.at[kind, source],
                        recv_sem=recv.at[kind, source],
                        device_id=(seg, source),
                        device_id_type=MESH,
                    ).wait_recv()

    row = lax.broadcasted_iota(jnp.int32, (HEAD_DIM, HEAD_DIM), 0)
    col = lax.broadcasted_iota(jnp.int32, (HEAD_DIM, HEAD_DIM), 1)
    for h in range(heads):
        st_ref[h, :, :HEAD_DIM] = jnp.zeros((HEAD_DIM, HEAD_DIM), f32)
        st_ref[h, :, HEAD_DIM:] = jnp.where(row == col, 1.0, 0.0).astype(f32)
    for copy in own:
        copy.wait()
    tail_from = order[2 * n]
    joint = order[n - 1] // 2
    early = (qa, ka, va, ga)
    late = (qb, kb, vb, gb)

    def from_tail(place, cols):
        return jnp.where(seg == 0, 0.0, otail[tail_from].astype(f32)[:, cols])

    def from_early(place, cols):
        return early[place][joint, half - 16 :, :].astype(f32)[8:]

    def run(first, stop, bufs, prior):
        def one(b, carry):
            block_pair(
                heads, b, first, order, bufs, prior, me * heads,
                w_ref, rate_ref, o_ref, mh_ref, ml_ref, st_ref, x_ref,
            )
            return carry

        lax.fori_loop(first // PAIR, stop // PAIR, one, 0)

    arrived((0, 1, 2, 3, 10, 11, 12))
    run(0, n // 2, early, from_tail)
    arrived((4, 5, 6, 7))
    run(n // 2, n, late, from_early)
    arrived((8, 9))
    for copy in started:
        copy.wait_send()


def close_kernel(
    n, segs, heads, order, end_ref, o_ref, mh_ref, ml_ref, z_ref, gain_ref, out,
    inc_ref, pass_ref, y_ref, send, recv, ysend, yrecv, local
):
    seg = lax.axis_index("seg")
    me = lax.axis_index("cp")
    final = segs - 1
    width = heads * HEAD_DIM
    def hop(h):
        return pltpu.make_async_remote_copy(
            src_ref=pass_ref.at[h],
            dst_ref=inc_ref.at[h],
            send_sem=send.at[h],
            recv_sem=recv.at[h],
            device_id=(lax.rem(seg + 1, segs), me),
            device_id_type=MESH,
        )

    @pl.when(seg == 0)
    def _():
        for h in range(heads):
            inc_ref[h] = jnp.zeros((HEAD_DIM, HEAD_DIM), f32)
            pass_ref[h] = end_ref[h, :, :HEAD_DIM]
        for h in range(heads):
            hop(h).start()

    @pl.when((seg > 0) & (seg < final))
    def _():
        for h in range(heads):
            through = split(end_ref[h, :, HEAD_DIM:])
            hop(h).wait_recv()
            pass_ref[h] = end_ref[h, :, :HEAD_DIM] + mm(through, split(inc_ref[h]))
            hop(h).start()

    def block(h, b, state):
        cols = pl.ds(h * HEAD_DIM, HEAD_DIM)
        i0 = order[2 * b]
        i1 = order[2 * b + 1]
        core = o_ref[h, b] + mm((mh_ref[h, b], ml_ref[h, b]), state)
        z = jnp.concatenate([z_ref[i0, :, cols], z_ref[i1, :, cols]], axis=0).astype(f32)
        scale = lax.rsqrt(jnp.sum(core * core, axis=-1, keepdims=True) * (1.0 / HEAD_DIM) + 1e-06)
        y_ref[h, b] = (core * scale * gain_ref[0:1, :] * (z / (1.0 + jnp.exp(-z)))).astype(bf16)

    def target(h, source):
        return out.at[:, pl.ds(pl.multiple_of(source * width + h * HEAD_DIM, HEAD_DIM), HEAD_DIM)]

    def give(h, d):
        peer = lax.rem(me + d, n)
        return pltpu.make_async_remote_copy(
            src_ref=y_ref.at[h, peer],
            dst_ref=target(h, me),
            send_sem=ysend.at[h, peer],
            recv_sem=yrecv.at[h, me],
            device_id=(seg, peer),
            device_id_type=MESH,
        )

    for h in range(heads):
        @pl.when(seg == final)
        def _():
            hop(h).wait_recv()

        state = split(inc_ref[h])

        for d in range(1, n):
            block(h, lax.rem(me + d, n), state)
            if d > 1:
                give(h, d - 1).start()
        block(h, me, state)
        give(h, n - 1).start()
        if h:
            pltpu.make_async_copy(y_ref.at[h - 1, me], target(h - 1, me), local.at[h - 1]).start()
    pltpu.make_async_copy(y_ref.at[heads - 1, me], target(heads - 1, me), local.at[heads - 1]).start()

    for h in range(heads):
        pltpu.make_async_copy(y_ref.at[h, me], target(h, me), local.at[h]).wait()
        for d in range(1, n):
            source = lax.rem(me + n - d, n)
            pltpu.make_async_remote_copy(
                src_ref=y_ref.at[h, source],
                dst_ref=target(h, source),
                send_sem=ysend.at[h, source],
                recv_sem=yrecv.at[h, source],
                device_id=(seg, source),
                device_id_type=MESH,
            ).wait_recv()
    for h in range(heads):
        for d in range(1, n):
            give(h, d).wait_send()

        @pl.when(seg < final)
        def _():
            hop(h).wait_send()


def whole_kernel(
    n, segs, heads, order, qkv, z, gates, conv_weight, rate_ref, gain_ref, out,
    o_ref, mh_ref, ml_ref, st_ref, oz, inc_ref, pass_ref, y_ref, *rest
):
    bufs, sems = rest[:11], rest[11:]
    mix_kernel(
        n, segs, heads, order, qkv, z, gates, conv_weight, rate_ref,
        o_ref, mh_ref, ml_ref, st_ref, oz, *bufs, *sems[:3],
    )
    close_kernel(
        n, segs, heads, order, st_ref, o_ref, mh_ref, ml_ref, oz, gain_ref, out,
        inc_ref, pass_ref, y_ref, *sems[3:],
    )


def mixer(n, segs, heads, order, qkv, z, gates, conv_weight, rates, gain):
    keys = max(1, heads // GROUP)
    wk, wv = keys * HEAD_DIM, heads * HEAD_DIM
    half = qkv.shape[0] // 2
    anywhere = pl.BlockSpec(memory_space=pl.ANY)
    vmem = pl.BlockSpec(memory_space=pltpu.VMEM)
    widths = (wk, wk, wv, gates.shape[1])
    square = (HEAD_DIM, HEAD_DIM)
    DMA = pltpu.SemaphoreType.DMA
    return pl.pallas_call(
        functools.partial(whole_kernel, n, segs, heads),
        out_shape=jax.ShapeDtypeStruct((BLOCK, n * heads * HEAD_DIM), bf16),
        in_specs=[pl.BlockSpec(memory_space=pltpu.SMEM)] + [anywhere] * 4 + [vmem] * 2,
        out_specs=vmem,
        scratch_shapes=[
            pltpu.VMEM((heads, n, BLOCK, HEAD_DIM), f32),
            pltpu.VMEM((heads, n, BLOCK, HEAD_DIM), bf16),
            pltpu.VMEM((heads, n, BLOCK, HEAD_DIM), bf16),
            pltpu.VMEM((heads, HEAD_DIM, 2 * HEAD_DIM), f32),
            pltpu.VMEM((2 * n, half, wv), bf16),
            pltpu.VMEM((heads,) + square, f32),
            pltpu.VMEM((heads,) + square, f32),
            pltpu.VMEM((heads, n, BLOCK, HEAD_DIM), bf16),
        ]
        + [pltpu.VMEM((n, half, w), bf16) for w in widths]
        + [pltpu.VMEM((n, half, w), bf16) for w in widths]
        + [
            pltpu.VMEM((n, TAIL, 2 * wk + wv), bf16),
            pltpu.VMEM((CONV, 2 * wk + wv), f32),
            pltpu.VMEM((PAIR, BLOCK + 8, 2 * wk + wv), f32),
            DMA((13, n)),
            DMA((13, n)),
            DMA((13,)),
            DMA((heads,)),
            DMA((heads,)),
            DMA((heads, n)),
            DMA((heads, n)),
            DMA((heads,)),
        ],
        compiler_params=pltpu.CompilerParams(
            collective_id=0, has_side_effects=True, vmem_limit_bytes=56 * 1024 * 1024
        ),
        name="mixer",
    )(order, qkv, z, gates, conv_weight, rates, gain)


def per_device(mixed_qkv, gate_z, gate_logits, block_table, conv_weight, a_log, dt_bias, norm_gain):
    n = lax.axis_size("cp")
    segs = lax.axis_size("seg")
    heads = VALUE_HEADS // n
    blocks = 2 * n

    prior_table = lax.ppermute(block_table, "seg", [(i, (i + 1) % segs) for i in range(segs)])
    places = jnp.arange(blocks, dtype=jnp.int32)
    order = jnp.sum(
        jnp.where(block_table[0][None, :] == places[:, None], places[None, :], 0), axis=1, dtype=jnp.int32
    )
    tail_from = jnp.sum(jnp.where(prior_table[0] == blocks - 1, places, 0), dtype=jnp.int32) // 2
    order = jnp.concatenate([order, tail_from[None]])
    spare = HEAD_DIM - 2 * VALUE_HEADS
    rates = jnp.stack(
        [jnp.pad(-jnp.exp(a_log), (VALUE_HEADS, spare)), jnp.pad(dt_bias, (VALUE_HEADS, spare))]
    )
    return mixer(
        n, segs, heads, order, mixed_qkv, gate_z, gate_logits, conv_weight, rates, norm_gain[None, :]
    )


def solution(mesh):
    return jax.shard_map(
        per_device,
        mesh=mesh,
        in_specs=(
            P(("seg", "cp"), None),
            P(("seg", "cp"), None),
            P(("seg", "cp"), None),
            P("seg", None),
            P(),
            P(),
            P(),
            P(),
        ),
        out_specs=P(("seg", "cp"), None),
        check_vma=False,
    )
```
